32 devices in a mesh: dp: 4 (over y, z), ep: 8 (over x, core).
Axes of the slice: x: 4, y: 2, z: 2, core: 2. Of those that a mesh axis runs over, the one named last changes fastest.
The devices are a block of a 4x4x8 slice.
Arguments:
- tokens: bfloat16 [4096, 2560], P(('dp', 'ep')), parts along dimension 0
- expert_ids: int32 [4096, 6], P(('dp', 'ep')), parts along dimension 0
- gate_vals: float32 [4096, 6], P(('dp', 'ep')), parts along dimension 0
- w_gate: bfloat16 [64, 2560, 1536], P('ep')
- w_up: bfloat16 [64, 2560, 1536], P('ep')
- w_down: bfloat16 [64, 1536, 2560], P('ep')
- shared_gate: bfloat16 [2560, 3072], replicated
- shared_up: bfloat16 [2560, 3072], replicated
- shared_down: bfloat16 [3072, 2560], replicated
Outputs:
- output: bfloat16 [4096, 2560], P(('dp', 'ep')), parts along dimension 0
There are 4 independent parts. The reference program is written for one: setup_inputs(seed, part) draws one part's arguments, and reference() takes and returns one part's arrays. A program takes and returns all parts, laid end to end along the dimension named above; an argument that names none is the same for every part.
All inputs are finite; a program needn't handle non-finite values.
Results may differ from the reference program's by a relative error of at most 0.00669141.
Values are sent between devices in bfloat16 or wider.
A program may use at most 768 MiB of HBM per device.

```python
import jax
import jax.numpy as jnp
from jax import lax

GROUP_SIZE = 8
TOKENS_DEV = 128
MODEL_DIM = 2560
EXPERT_FF = 1536
SHARED_FF = 3072
EXPERTS = 64
TOP_K = 6
LOCAL_EXPERTS = EXPERTS // GROUP_SIZE
SPREAD_SLOTS = max(GROUP_SIZE, EXPERTS // 2)
CAPACITY = (TOKENS_DEV * TOP_K + SPREAD_SLOTS - 1) // SPREAD_SLOTS


def route_ids(route_key):
    key_shift, key_base, key_perm = jax.random.split(route_key, 3)
    dev_shift = jax.random.randint(key_shift, (GROUP_SIZE, 1, 1), 0, GROUP_SIZE)
    base_local = jax.random.randint(key_base, (), 0, LOCAL_EXPERTS)
    src_index = jnp.arange(GROUP_SIZE, dtype=jnp.int32).reshape(GROUP_SIZE, 1, 1)
    local_shift = base_local + src_index * (SPREAD_SLOTS // GROUP_SIZE)
    perm_keys = jax.random.split(key_perm, GROUP_SIZE)
    tok_order = jax.vmap(lambda perm_key: jax.random.permutation(perm_key, TOKENS_DEV))(perm_keys)
    row_pos = tok_order[:, :, None] * TOP_K + jnp.arange(TOP_K, dtype=jnp.int32).reshape(1, 1, TOP_K)
    spot_idx = row_pos % SPREAD_SLOTS
    dest_dev = (dev_shift + spot_idx) % GROUP_SIZE
    local_id = (local_shift + spot_idx // GROUP_SIZE) % LOCAL_EXPERTS
    return (dest_dev * LOCAL_EXPERTS + local_id).reshape(GROUP_SIZE * TOKENS_DEV, TOP_K).astype(jnp.int32)


def setup_inputs(seed: int = 0, part: int = 0) -> dict:
    part_key = jax.random.fold_in(jax.random.key(seed), part)
    key_tok, key_route, key_gate = jax.random.split(part_key, 3)
    weight_keys = jax.random.split(jax.random.key(seed + 1), 6)
    row_count = GROUP_SIZE * TOKENS_DEV
    tokens = jax.random.normal(key_tok, (row_count, MODEL_DIM), jnp.float32).astype(jnp.bfloat16)
    expert_ids = route_ids(key_route)
    gate_vals = 3.0 * TOP_K ** -0.5 * jax.nn.sigmoid(2.0 * jax.random.normal(key_gate, (row_count, TOP_K), jnp.float32))
    w_gate = (jax.random.normal(weight_keys[0], (EXPERTS, MODEL_DIM, EXPERT_FF), jnp.float32) * MODEL_DIM ** -0.5).astype(jnp.bfloat16)
    w_up = (jax.random.normal(weight_keys[1], (EXPERTS, MODEL_DIM, EXPERT_FF), jnp.float32) * MODEL_DIM ** -0.5).astype(jnp.bfloat16)
    w_down = (jax.random.normal(weight_keys[2], (EXPERTS, EXPERT_FF, MODEL_DIM), jnp.float32) * EXPERT_FF ** -0.5).astype(jnp.bfloat16)
    shared_gate = (jax.random.normal(weight_keys[3], (MODEL_DIM, SHARED_FF), jnp.float32) * MODEL_DIM ** -0.5).astype(jnp.bfloat16)
    shared_up = (jax.random.normal(weight_keys[4], (MODEL_DIM, SHARED_FF), jnp.float32) * MODEL_DIM ** -0.5).astype(jnp.bfloat16)
    shared_down = (jax.random.normal(weight_keys[5], (SHARED_FF, MODEL_DIM), jnp.float32) * SHARED_FF ** -0.5).astype(jnp.bfloat16)
    return {"tokens": tokens, "expert_ids": expert_ids, "gate_vals": gate_vals, "w_gate": w_gate, "w_up": w_up, "w_down": w_down, "shared_gate": shared_gate, "shared_up": shared_up, "shared_down": shared_down}


def swiglu(row_block, gate_w, up_w, down_w):
    gate_act = jnp.dot(row_block, gate_w, preferred_element_type=jnp.float32)
    up_act = jnp.dot(row_block, up_w, preferred_element_type=jnp.float32)
    hidden = (jax.nn.silu(gate_act) * up_act).astype(jnp.bfloat16)
    return jnp.dot(hidden, down_w, preferred_element_type=jnp.float32).astype(jnp.bfloat16)


def reference(tokens, expert_ids, gate_vals, w_gate, w_up, w_down, shared_gate, shared_up, shared_down):
    row_count = GROUP_SIZE * TOKENS_DEV
    src_ids = expert_ids.reshape(GROUP_SIZE, TOKENS_DEV * TOP_K)
    one_hot = (src_ids[:, :, None] == jnp.arange(EXPERTS, dtype=jnp.int32)[None, None, :]).astype(jnp.int32)
    slot_pos = jnp.sum(jnp.cumsum(one_hot, axis=1) * one_hot, axis=2) - 1
    buf_row = (jnp.arange(GROUP_SIZE, dtype=jnp.int32)[:, None] * CAPACITY + slot_pos).reshape(-1)
    flat_ids = src_ids.reshape(-1)
    token_rows = jnp.repeat(tokens, TOP_K, axis=0)
    buffers = jnp.zeros((EXPERTS, GROUP_SIZE * CAPACITY, MODEL_DIM), jnp.bfloat16)
    buffers = buffers.at[flat_ids, buf_row].set(token_rows)
    expert_out = lax.map(lambda operands: swiglu(operands[0], operands[1], operands[2], operands[3]), (buffers, w_gate, w_up, w_down))
    picked = expert_out[flat_ids, buf_row].reshape(row_count, TOP_K, MODEL_DIM)
    result_acc = tokens.astype(jnp.float32)
    for slot_idx in range(TOP_K):
        result_acc = result_acc + gate_vals[:, slot_idx:slot_idx + 1] * picked[:, slot_idx, :].astype(jnp.float32)
    shared_out = swiglu(tokens, shared_gate, shared_up, shared_down)
    return (result_acc + shared_out.astype(jnp.float32)).astype(jnp.bfloat16)
```

```python
import functools

import jax
import jax.numpy as jnp
from jax import lax
from jax.experimental import pallas as pl
from jax.experimental.pallas import tpu as pltpu
from jax.sharding import PartitionSpec as P

F32 = jnp.float32
BF16 = jnp.bfloat16
NS = 5
NC = 5


def moe_kernel(dims, ids_ref, gates_ref, tok, wg, wu, wd, sg, su, sd, out_ref,
               xall, xown, xg, acc, h, y, pst, dsum, hrecv, frecv, oh, gt, hs, sgacc, shr, posr, grecv, gsend, slots,
               slot_sem, loc_sem, g_ssem, g_rsem, a_ssem, a_rsem, d_ssem, d_rsem, h_ssem, h_rsem, f_ssem, f_rsem):
    ng, nq, T, D, F, SF, E, cap, top = dims
    W = D // NC
    TC = W // 2
    NT = D // TC
    R = 2 * cap
    M = nq * R
    HT = T // 2
    FJ = F // W
    SFJ = SF // W
    n1 = NC * E
    ntot = n1 + 2 * NT + 2 * SFJ + NC

    me = lax.axis_index("ep")
    q = me // 2
    k = lax.rem(me, 2)
    lq = lax.rem(q + nq - 1, nq)
    rq = lax.rem(q + 1, nq)
    oq = lax.rem(q + 2, nq)
    sib = 2 * q + 1 - k
    left = 2 * lq + k
    right = 2 * rq + k
    opp = 2 * oq + k

    def rc(src, dst, ssem, rsem, dev):
        return pltpu.make_async_remote_copy(src_ref=src, dst_ref=dst, send_sem=ssem, recv_sem=rsem,
                                            device_id={"ep": dev}, device_id_type=pl.DeviceIdType.MESH)

    def issue(n):
        sl = lax.rem(n, NS)
        sem = slot_sem.at[sl]

        @pl.when(n < n1)
        def _():
            c = n // E
            e = lax.rem(n, E)
            for j in range(FJ):
                pltpu.make_async_copy(wg.at[e, pl.ds(pl.multiple_of(c * W, W), W), pl.ds(j * W, W)],
                                      slots.at[sl, pl.ds(j * W, W), :], sem).start()
            for j in range(FJ):
                pltpu.make_async_copy(wu.at[e, pl.ds(pl.multiple_of(c * W, W), W), pl.ds(j * W, W)],
                                      slots.at[sl, pl.ds((FJ + j) * W, W), :], sem).start()

        m = n - n1
        last = n >= ntot - 2
        r = lax.rem(m, 4)
        ct = jnp.where(last, NT - 1, m // 4)
        half = jnp.where(last, n - (ntot - 2), r)

        @pl.when((n >= n1) & (n < ntot) & ((r < 2) | last))
        def _():
            for j in range(E // 2):
                pltpu.make_async_copy(wd.at[half * (E // 2) + j, :, pl.ds(pl.multiple_of(ct * TC, TC), TC)],
                                      slots.at[sl, pl.ds((j // 2) * F, F), pl.ds((j % 2) * TC, TC)], sem).start()

        s = 2 * (m // 4) + r - 2
        shared = (n >= n1) & (n < ntot - 2) & (r >= 2)
        fcol = pl.ds(pl.multiple_of((s // 2) * W, W), W)

        @pl.when(shared & (s < 2 * SFJ) & (lax.rem(s, 2) == 0))
        def _():
            pltpu.make_async_copy(sg.at[:, fcol], slots.at[sl, pl.ds(0, D), :], sem).start()

        @pl.when(shared & (s < 2 * SFJ) & (lax.rem(s, 2) == 1))
        def _():
            pltpu.make_async_copy(su.at[:, fcol], slots.at[sl, pl.ds(0, D), :], sem).start()

        @pl.when(shared & (s >= 2 * SFJ))
        def _():
            col = pl.ds(pl.multiple_of((s - 2 * SFJ) * W, W), W)
            pltpu.make_async_copy(sd.at[:, col], slots.at[sl], sem).start()

    def wait_full(sl):
        pltpu.make_async_copy(sd.at[:, pl.ds(0, W)], slots.at[sl], slot_sem.at[sl]).wait()

    def wait_gu(sl):
        pltpu.make_async_copy(sg.at[:, pl.ds(0, W)], slots.at[sl, pl.ds(0, D), :], slot_sem.at[sl]).wait()

    xcopies = [pltpu.make_async_copy(tok.at[:, pl.ds(c * W, W)], xall.at[c, me], loc_sem.at[c]) for c in range(NC)]
    xcopies.append(pltpu.make_async_copy(tok, xown, loc_sem.at[NC]))
    for cp in xcopies:
        cp.start()
    for n in range(NS):
        issue(jnp.int32(n))

    eiota = lax.broadcasted_iota(jnp.int32, (ng * E, T), 0)
    dense = jnp.zeros((ng * E, T), F32)
    for j in range(top):
        dense = dense + jnp.where(ids_ref[j:j + 1, :] == eiota, gates_ref[j:j + 1, :], 0.0)
    gsend[...] = dense.reshape(ng, E, T)

    bar = pltpu.get_barrier_semaphore()
    for i in range(1, ng):
        pl.semaphore_signal(bar, inc=1, device_id={"ep": lax.rem(me + i, ng)}, device_id_type=pl.DeviceIdType.MESH)
    pl.semaphore_wait(bar, ng - 1)

    lo, hi = pl.ds(0, HT), pl.ds(HT, HT)

    def ag(c, typ, dev, src_dev, rows, dst_dev=None):
        ref = xall.at[c, src_dev] if rows is None else xall.at[c, src_dev, rows, :]
        return rc(ref, ref, a_ssem.at[c, typ], a_rsem.at[c, typ], dev)

    def own(c):
        ag(c, 0, right, me, lo).start()
        ag(c, 2, left, me, hi).start()
        ag(c, 1, right, me, hi).start()
        ag(c, 3, left, me, lo).start()
        ag(c, 6, sib, me, None).start()

    def svc0(c):
        ag(c, 0, left, left, lo).wait_recv()
        ag(c, 4, right, left, lo).start()
        ag(c, 2, right, right, hi).wait_recv()
        ag(c, 5, left, right, hi).start()

        @pl.when(c + 1 < NC)
        def _():
            own(c + 1)

    def svc1(c):
        ag(c, 1, left, left, hi).wait_recv()
        ag(c, 7, sib, left, None).start()
        ag(c, 3, right, right, lo).wait_recv()
        ag(c, 8, sib, right, None).start()

    def svc2(c):
        ag(c, 4, left, opp, lo).wait_recv()
        ag(c, 5, right, opp, hi).wait_recv()
        ag(c, 9, sib, opp, None).start()

    def need(c):
        sl_, sr_, so_ = 2 * lq + 1 - k, 2 * rq + 1 - k, 2 * oq + 1 - k
        ag(c, 6, sib, sib, None).wait_recv()
        ag(c, 7, sib, sl_, None).wait_recv()
        ag(c, 8, sib, sr_, None).wait_recv()
        ag(c, 9, sib, so_, None).wait_recv()

    for c in range(NC):
        xcopies[c].wait()
    own(jnp.int32(0))
    for i in range(1, ng):
        d = lax.rem(me + i, ng)
        rc(gsend.at[d], grecv.at[me], g_ssem.at[i], g_rsem.at[i], d).start()

    for e in range(E):
        acc[e] = jnp.zeros((M, 2 * F), F32)

    svc0(jnp.int32(0))

    for i in range(1, ng):
        s = lax.rem(me + ng - i, ng)
        rc(gsend.at[s], grecv.at[s], g_ssem.at[i], g_rsem.at[i], s).wait_recv()
    grecv[me] = gsend[me]
    gall = grecv[...].reshape(ng * E, T)
    mask = gall > 0.0
    tri = (lax.broadcasted_iota(jnp.int32, (T, T), 0) < lax.broadcasted_iota(jnp.int32, (T, T), 1)).astype(F32).astype(BF16)
    pos = jnp.dot(mask.astype(F32).astype(BF16), tri, preferred_element_type=F32)
    posr[...] = jnp.where(mask, pos, -1000.0).reshape(ng, E, T)

    svc1(jnp.int32(0))

    riota = lax.broadcasted_iota(jnp.int32, (R, T), 0).astype(F32)

    def route(b, _):
        parts = []
        for e in range(E):
            hits, gs = [], []
            for s in range(2):
                hit = posr[2 * b + s, e:e + 1, :] == (riota - float(s * cap))
                hits.append(jnp.where(hit, 1.0, 0.0))
                gs.append(jnp.where(hit, grecv[2 * b + s, e:e + 1, :], 0.0))
            oh[b, e] = jnp.concatenate(hits, axis=1).astype(BF16)
            parts.append(jnp.concatenate(gs, axis=1))
        g = jnp.concatenate(parts, axis=0).T
        g0 = g.astype(BF16)
        rem = g - g0.astype(F32)
        g1 = rem.astype(BF16)
        gt[b, 0] = g0
        gt[b, 1] = g1
        gt[b, 2] = (rem - g1.astype(F32)).astype(BF16)
        return 0

    lax.fori_loop(0, nq, route, 0)
    svc2(jnp.int32(0))

    def chunk(c, _):
        need(c)
        for b in range(nq):
            ohb = oh[b].reshape(E * R, 2 * T)
            xb = xall[c, 2 * b:2 * b + 2].reshape(2 * T, W)
            rows = jnp.dot(ohb, xb, preferred_element_type=F32).astype(BF16)
            xg[:, b * R:(b + 1) * R, :] = rows.reshape(E, R, W)

        def estep(e, _):
            n = c * E + e
            sl = lax.rem(n, NS)
            wait_full(sl)
            xe = xg[e]
            for j in range(2 * FJ):
                acc[e, :, j * W:(j + 1) * W] += jnp.dot(xe, slots[sl, j * W:(j + 1) * W, :], preferred_element_type=F32)
            issue(n + NS)

            @pl.when(c == NC - 1)
            def _():
                for j in range(FJ):
                    gv = acc[e, :, j * W:(j + 1) * W]
                    uv = acc[e, :, F + j * W:F + (j + 1) * W]
                    h[e, :, j * W:(j + 1) * W] = (gv * jax.nn.sigmoid(gv) * uv).astype(BF16)

            @pl.when((c < NC - 1) & (e == 1))
            def _():
                svc0(c + 1)

            @pl.when((c < NC - 1) & (e == 3))
            def _():
                svc1(c + 1)

            @pl.when((c < NC - 1) & (e == E - 2))
            def _():
                svc2(c + 1)
            return 0

        lax.fori_loop(0, E, estep, 0)
        return 0

    lax.fori_loop(0, NC, chunk, 0)

    def dcopy(ct, buf, dev):
        return rc(pst.at[buf, 1 - k], dsum.at[ct], d_ssem.at[ct], d_rsem.at[ct], dev)

    def hcopy(ct, i):
        rows = (lo, hi)[i]
        return rc(dsum.at[ct, oq, rows, :], hrecv.at[ct, i], h_ssem.at[ct, i], h_rsem.at[ct, i], (right, left)[i])

    def fcopy(ct, i):
        return rc(dsum.at[ct, (rq, lq)[i]], frecv.at[ct, i], f_ssem.at[ct, i], f_rsem.at[ct, i], (right, left)[i])

    def svca(ct):
        dcopy(ct, lax.rem(ct, 2), sib).wait_recv()
        for d in (oq, rq, lq, q):
            dsum[ct, d] += pst[lax.rem(ct, 2), k, d]
        hcopy(ct, 0).start()
        hcopy(ct, 1).start()

    def svcb(ct):
        hcopy(ct, 0).wait_recv()
        dsum[ct, rq, :HT, :] += hrecv[ct, 0]
        fcopy(ct, 0).start()
        hcopy(ct, 1).wait_recv()
        dsum[ct, lq, HT:, :] += hrecv[ct, 1]
        fcopy(ct, 1).start()

    def svcc(ct, _):
        fcopy(ct, 0).wait_recv()
        fcopy(ct, 1).wait_recv()
        cols = pl.ds(pl.multiple_of(ct * TC, TC), TC)
        routed = dsum[ct, q] + frecv[ct, 0] + frecv[ct, 1]
        out_ref[:, cols] = (xown[:, cols].astype(F32) + routed + shr[:, cols].astype(F32)).astype(BF16)
        return 0

    def shared_step(s, n):
        sl = lax.rem(n, NS)
        fcol = pl.ds(pl.multiple_of((s // 2) * W, W), W)

        @pl.when((s < 2 * SFJ) & (lax.rem(s, 2) == 0))
        def _():
            wait_gu(sl)
            sgacc[...] = jnp.dot(xown[...], slots[sl, :D, :], preferred_element_type=F32)

        @pl.when((s < 2 * SFJ) & (lax.rem(s, 2) == 1))
        def _():
            wait_gu(sl)
            uv = jnp.dot(xown[...], slots[sl, :D, :], preferred_element_type=F32)
            gv = sgacc[...]
            hs[:, fcol] = (gv * jax.nn.sigmoid(gv) * uv).astype(BF16)

        @pl.when(s >= 2 * SFJ)
        def _():
            wait_full(sl)
            col = pl.ds(pl.multiple_of((s - 2 * SFJ) * W, W), W)
            shr[:, col] = jnp.dot(hs[...], slots[sl], preferred_element_type=F32).astype(BF16)

        issue(n + NS)

    xcopies[NC].wait()

    def tile(ct, _):
        buf = lax.rem(ct, 2)
        base = n1 + 4 * ct - jnp.where(ct == NT - 1, 1, 0)

        def dstep(half, _):
            n = base + half
            sl = lax.rem(n, NS)
            wait_full(sl)
            for j in range(E // 2):
                e = half * (E // 2) + j
                w = slots[sl, (j // 2) * F:(j // 2 + 1) * F, (j % 2) * TC:(j % 2 + 1) * TC]
                ye = jnp.dot(h[e], w, preferred_element_type=F32).astype(BF16)
                y[:, e] = ye.reshape(nq, R, TC)
            issue(n + NS)
            return 0

        lax.fori_loop(0, 2, dstep, 0)

        @pl.when(ct >= 2)
        def _():
            dcopy(ct - 2, buf, sib).wait_send()

        def combine(b, _):
            yb = y[b].reshape(E * R, TC)
            p = jnp.dot(gt[b, 0], yb, preferred_element_type=F32)
            p = p + jnp.dot(gt[b, 1], yb, preferred_element_type=F32)
            p = p + jnp.dot(gt[b, 2], yb, preferred_element_type=F32)
            pst[buf, 0, b] = p[:T]
            pst[buf, 1, b] = p[T:]
            return 0

        lax.fori_loop(0, nq, combine, 0)
        dcopy(ct, buf, sib).start()

        @pl.when(ct < NT - 1)
        def _():
            shared_step(2 * ct, base + 2)

        svca(ct)

        @pl.when(ct >= 1)
        def _():
            svcb(ct - 1)

        @pl.when(ct < NT - 2)
        def _():
            shared_step(2 * ct + 1, base + 3)
        return 0

    lax.fori_loop(0, NT, tile, 0)
    lax.fori_loop(0, NT - 4, svcc, 0)
    svcb(jnp.int32(NT - 1))
    lax.fori_loop(NT - 4, NT, svcc, 0)

    for i in range(1, ng):
        d = lax.rem(me + i, ng)
        rc(gsend.at[d], grecv.at[me], g_ssem.at[i], g_rsem.at[i], d).wait_send()

    def drain_ag(c, _):
        for typ, rows in ((0, lo), (1, hi), (2, hi), (3, lo), (4, lo), (5, hi), (6, None), (7, None), (8, None), (9, None)):
            ag(c, typ, sib, me, rows).wait_send()
        return 0

    lax.fori_loop(0, NC, drain_ag, 0)

    def drain_rs(ct, _):
        @pl.when(ct >= NT - 2)
        def _():
            dcopy(ct, lax.rem(ct, 2), sib).wait_send()
        for i in range(2):
            hcopy(ct, i).wait_send()
            fcopy(ct, i).wait_send()
        return 0

    lax.fori_loop(0, NT, drain_rs, 0)


def solution(mesh):
    ng = mesh.shape["ep"]
    nq = ng // 2

    def moe_step(tokens, expert_ids, gate_vals, w_gate, w_up, w_down, shared_gate, shared_up, shared_down):
        T, D = tokens.shape
        top = expert_ids.shape[1]
        E, _, F = w_gate.shape
        SF = shared_gate.shape[1]
        spread = max(ng, E * ng // 2)
        cap = (T * top + spread - 1) // spread
        W = D // NC
        TC = W // 2
        NT = D // TC
        R = 2 * cap
        M = nq * R
        dims = (ng, nq, T, D, F, SF, E, cap, top)
        any_spec = pl.BlockSpec(memory_space=pl.ANY)
        vm_spec = pl.BlockSpec(memory_space=pltpu.VMEM)
        dma = pltpu.SemaphoreType.DMA
        flops = 2 * 3 * D * (E * M * F + T * SF)
        return pl.pallas_call(
            functools.partial(moe_kernel, dims),
            out_shape=jax.ShapeDtypeStruct((T, D), BF16),
            in_specs=[vm_spec, vm_spec] + [any_spec] * 7,
            out_specs=vm_spec,
            scratch_shapes=[
                pltpu.VMEM((NC, ng, T, W), BF16),
                pltpu.VMEM((T, D), BF16),
                pltpu.VMEM((E, M, W), BF16),
                pltpu.VMEM((E, M, 2 * F), F32),
                pltpu.VMEM((E, M, F), BF16),
                pltpu.VMEM((nq, E, R, TC), BF16),
                pltpu.VMEM((2, 2, nq, T, TC), F32),
                pltpu.VMEM((NT, nq, T, TC), F32),
                pltpu.VMEM((NT, 2, T // 2, TC), F32),
                pltpu.VMEM((NT, 2, T, TC), F32),
                pltpu.VMEM((nq, E, R, 2 * T), BF16),
                pltpu.VMEM((nq, 3, 2 * T, E * R), BF16),
                pltpu.VMEM((T, SF), BF16),
                pltpu.VMEM((T, W), F32),
                pltpu.VMEM((T, D), BF16),
                pltpu.VMEM((ng, E, T), F32),
                pltpu.VMEM((ng, E, T), F32),
                pltpu.VMEM((ng, E, T), F32),
                pltpu.VMEM((NS, SF, W), BF16),
                dma((NS,)), dma((NC + 1,)), dma((ng,)), dma((ng,)),
                dma((NC, 10)), dma((NC, 10)), dma((NT,)), dma((NT,)),
                dma((NT, 2)), dma((NT, 2)), dma((NT, 2)), dma((NT, 2)),
            ],
            compiler_params=pltpu.CompilerParams(collective_id=0, has_side_effects=True, vmem_limit_bytes=67043328),
            cost_estimate=pl.CostEstimate(flops=flops, bytes_accessed=2 * 3 * D * (E * F + SF), transcendentals=0),
        )(expert_ids.T, gate_vals.T, tokens, w_gate, w_up, w_down, shared_gate, shared_up, shared_down)

    row_spec = P(("dp", "ep"), None)
    expert_spec = P("ep", None, None)
    whole_spec = P(None, None)
    return jax.shard_map(moe_step, mesh=mesh, in_specs=(row_spec, row_spec, row_spec, expert_spec, expert_spec, expert_spec, whole_spec, whole_spec, whole_spec), out_specs=row_spec, check_vma=False)
```

```python
import functools

import jax
import jax.numpy as jnp
from jax import lax
from jax.experimental import pallas as pl
from jax.experimental.pallas import tpu as pltpu
from jax.sharding import PartitionSpec as P

F32 = jnp.float32
BF16 = jnp.bfloat16
NS = 5
NC = 5
KS = 8


def moe_kernel(dims, ids_ref, gates_ref, tok, wg, wu, wd, sg, su, sd, out_ref,
               xall, xown, xg, acc, h, y, pst, dsum, rmsg, oh, gt, hs, sgacc, shr, posr, grecv, gsend, slots,
               slot_sem, loc_sem, g_ssem, g_rsem, a_ssem, a_rsem, d_ssem, d_rsem, m_ssem, m_rsem):
    ng, nq, T, D, F, SF, E, cap, top = dims
    W = D // NC
    TC = W // 2
    NT = D // TC
    R = 2 * cap
    M = nq * R
    HT = T // 2
    FJ = F // W
    SFJ = SF // W
    n1 = KS + NC * E
    ns = 2 * SFJ + NC
    ntot = KS + NC * E + 2 * NT + ns - KS
    nm = NT + 2
    MR = HT + T

    me = lax.axis_index("ep")
    q = me // 2
    k = lax.rem(me, 2)
    lq = lax.rem(q + nq - 1, nq)
    rq = lax.rem(q + 1, nq)
    oq = lax.rem(q + 2, nq)
    sib = 2 * q + 1 - k
    left = 2 * lq + k
    right = 2 * rq + k
    opp = 2 * oq + k

    def rc(src, dst, ssem, rsem, dev):
        return pltpu.make_async_remote_copy(src_ref=src, dst_ref=dst, send_sem=ssem, recv_sem=rsem,
                                            device_id={"ep": dev}, device_id_type=pl.DeviceIdType.MESH)

    def issue(n):
        sl = lax.rem(n, NS)
        sem = slot_sem.at[sl]

        @pl.when((n >= KS) & (n < n1))
        def _():
            c = (n - KS) // E
            e = lax.rem(n - KS, E)
            for j in range(FJ):
                pltpu.make_async_copy(wg.at[e, pl.ds(pl.multiple_of(c * W, W), W), pl.ds(j * W, W)],
                                      slots.at[sl, pl.ds(j * W, W), :], sem).start()
            for j in range(FJ):
                pltpu.make_async_copy(wu.at[e, pl.ds(pl.multiple_of(c * W, W), W), pl.ds(j * W, W)],
                                      slots.at[sl, pl.ds((FJ + j) * W, W), :], sem).start()

        m = jnp.maximum(n - n1, 0)
        ct = m // 3
        half = lax.rem(m, 3)

        @pl.when((n >= n1) & (n < ntot) & (half < 2))
        def _():
            for j in range(E // 2):
                pltpu.make_async_copy(wd.at[half * (E // 2) + j, :, pl.ds(pl.multiple_of(ct * TC, TC), TC)],
                                      slots.at[sl, pl.ds((j // 2) * F, F), pl.ds((j % 2) * TC, TC)], sem).start()

        s = jnp.where(n < KS, n, KS + ct)
        shared = (n < KS) | ((n >= n1) & (n < ntot) & (half == 2))
        fcol = pl.ds(pl.multiple_of((s // 2) * W, W), W)

        @pl.when(shared & (s < 2 * SFJ) & (lax.rem(s, 2) == 0))
        def _():
            pltpu.make_async_copy(sg.at[:, fcol], slots.at[sl, pl.ds(0, D), :], sem).start()

        @pl.when(shared & (s < 2 * SFJ) & (lax.rem(s, 2) == 1))
        def _():
            pltpu.make_async_copy(su.at[:, fcol], slots.at[sl, pl.ds(0, D), :], sem).start()

        @pl.when(shared & (s >= 2 * SFJ))
        def _():
            col = pl.ds(pl.multiple_of((s - 2 * SFJ) * W, W), W)
            pltpu.make_async_copy(sd.at[:, col], slots.at[sl], sem).start()

    def wait_full(sl):
        pltpu.make_async_copy(sd.at[:, pl.ds(0, W)], slots.at[sl], slot_sem.at[sl]).wait()

    def wait_gu(sl):
        pltpu.make_async_copy(sg.at[:, pl.ds(0, W)], slots.at[sl, pl.ds(0, D), :], slot_sem.at[sl]).wait()

    xcopies = [pltpu.make_async_copy(tok.at[:, pl.ds(c * W, W)], xall.at[c, me], loc_sem.at[c]) for c in range(NC)]
    xcopies.append(pltpu.make_async_copy(tok, xown, loc_sem.at[NC]))
    for cp in xcopies:
        cp.start()
    for n in range(NS):
        issue(jnp.int32(n))

    eiota = lax.broadcasted_iota(jnp.int32, (ng * E, T), 0)
    dense = jnp.zeros((ng * E, T), F32)
    for j in range(top):
        dense = dense + jnp.where(ids_ref[j:j + 1, :] == eiota, gates_ref[j:j + 1, :], 0.0)
    gsend[...] = dense.reshape(ng, E, T)

    bar = pltpu.get_barrier_semaphore()
    for i in range(1, ng):
        pl.semaphore_signal(bar, inc=1, device_id={"ep": lax.rem(me + i, ng)}, device_id_type=pl.DeviceIdType.MESH)
    pl.semaphore_wait(bar, ng - 1)

    lo, hi = pl.ds(0, HT), pl.ds(HT, HT)

    def ag(c, typ, dev, src_dev, rows, dst_dev=None):
        ref = xall.at[c, src_dev] if rows is None else xall.at[c, src_dev, rows, :]
        return rc(ref, ref, a_ssem.at[c, typ], a_rsem.at[c, typ], dev)

    def own(c):
        ag(c, 0, right, me, lo).start()
        ag(c, 2, left, me, hi).start()
        ag(c, 1, right, me, hi).start()
        ag(c, 3, left, me, lo).start()
        ag(c, 6, sib, me, None).start()

    def svc0(c):
        ag(c, 0, left, left, lo).wait_recv()
        ag(c, 4, right, left, lo).start()
        ag(c, 2, right, right, hi).wait_recv()
        ag(c, 5, left, right, hi).start()

    def svc1(c):
        ag(c, 1, left, left, hi).wait_recv()
        ag(c, 7, sib, left, None).start()
        ag(c, 3, right, right, lo).wait_recv()
        ag(c, 8, sib, right, None).start()

    def svc2(c):
        ag(c, 4, left, opp, lo).wait_recv()
        ag(c, 5, right, opp, hi).wait_recv()
        ag(c, 9, sib, opp, None).start()

    def need(c):
        sl_, sr_, so_ = 2 * lq + 1 - k, 2 * rq + 1 - k, 2 * oq + 1 - k
        ag(c, 6, sib, sib, None).wait_recv()
        ag(c, 7, sib, sl_, None).wait_recv()
        ag(c, 8, sib, sr_, None).wait_recv()
        ag(c, 9, sib, so_, None).wait_recv()

    def shared_gu(s, n):
        sl = lax.rem(n, NS)
        fcol = pl.ds(pl.multiple_of((s // 2) * W, W), W)

        @pl.when(lax.rem(s, 2) == 0)
        def _():
            wait_gu(sl)
            sgacc[...] = jnp.dot(xown[...], slots[sl, :D, :], preferred_element_type=F32)

        @pl.when(lax.rem(s, 2) == 1)
        def _():
            wait_gu(sl)
            uv = jnp.dot(xown[...], slots[sl, :D, :], preferred_element_type=F32)
            gv = sgacc[...]
            hs[:, fcol] = (gv * jax.nn.sigmoid(gv) * uv).astype(BF16)

    def shared_step(s, n):
        sl = lax.rem(n, NS)

        @pl.when(s < 2 * SFJ)
        def _():
            shared_gu(s, n)

        @pl.when(s >= 2 * SFJ)
        def _():
            wait_full(sl)
            col = pl.ds(pl.multiple_of((s - 2 * SFJ) * W, W), W)
            shr[:, col] = jnp.dot(hs[...], slots[sl], preferred_element_type=F32).astype(BF16)

        issue(n + NS)

    def early(first, last):
        def body(n, _):
            shared_gu(n, n)
            issue(n + NS)
            return 0
        lax.fori_loop(first, last, body, 0)

    for c in range(NC):
        xcopies[c].wait()
    own(jnp.int32(0))
    for i in range(1, ng):
        d = lax.rem(me + i, ng)
        rc(gsend.at[d], grecv.at[me], g_ssem.at[i], g_rsem.at[i], d).start()

    xcopies[NC].wait()
    early(0, 3)
    for e in range(E):
        acc[e] = jnp.zeros((M, 2 * F), F32)
    early(3, 4)
    svc0(jnp.int32(0))
    early(4, 5)
    svc1(jnp.int32(0))

    for i in range(1, ng):
        s = lax.rem(me + ng - i, ng)
        rc(gsend.at[s], grecv.at[s], g_ssem.at[i], g_rsem.at[i], s).wait_recv()
    grecv[me] = gsend[me]
    gall = grecv[...].reshape(ng * E, T)
    mask = gall > 0.0
    tri = (lax.broadcasted_iota(jnp.int32, (T, T), 0) < lax.broadcasted_iota(jnp.int32, (T, T), 1)).astype(F32).astype(BF16)
    pos = jnp.dot(mask.astype(F32).astype(BF16), tri, preferred_element_type=F32)
    posr[...] = jnp.where(mask, pos, -1000.0).reshape(ng, E, T)

    riota = lax.broadcasted_iota(jnp.int32, (R, T), 0).astype(F32)
    ciota = lax.broadcasted_iota(jnp.int32, (cap, T), 0).astype(F32)

    def route(b, _):
        for e in range(E):
            hits = [jnp.where(posr[2 * b + s, e:e + 1, :] == (riota - float(s * cap)), 1.0, 0.0) for s in range(2)]
            oh[b, e] = jnp.concatenate(hits, axis=1).astype(BF16)
        for s in range(2):
            src = 2 * b + s
            g = jnp.concatenate([jnp.where(posr[src, e:e + 1, :] == ciota, grecv[src, e:e + 1, :], 0.0)
                                 for e in range(E)], axis=0).T
            g0 = g.astype(BF16)
            rem = g - g0.astype(F32)
            g1 = rem.astype(BF16)
            gt[src, :T] = g0
            gt[src, T:2 * T] = g1
            gt[src, 2 * T:] = (rem - g1.astype(F32)).astype(BF16)
        return 0

    lax.fori_loop(0, nq, route, 0)
    early(5, 6)
    svc2(jnp.int32(0))
    own(jnp.int32(1))
    early(6, KS)

    def chunk(c, _):
        need(c)
        for b in range(nq):
            ohb = oh[b].reshape(E * R, 2 * T)
            xb = xall[c, 2 * b:2 * b + 2].reshape(2 * T, W)
            rows = jnp.dot(ohb, xb, preferred_element_type=F32).astype(BF16)
            xg[:, b * R:(b + 1) * R, :] = rows.reshape(E, R, W)

        def estep(e, _):
            n = KS + c * E + e
            sl = lax.rem(n, NS)
            wait_full(sl)
            xe = xg[e]
            for j in range(2 * FJ):
                acc[e, :, j * W:(j + 1) * W] += jnp.dot(xe, slots[sl, j * W:(j + 1) * W, :], preferred_element_type=F32)
            issue(n + NS)

            @pl.when(c == NC - 1)
            def _():
                for j in range(FJ):
                    gv = acc[e, :, j * W:(j + 1) * W]
                    uv = acc[e, :, F + j * W:F + (j + 1) * W]
                    h[e, :, j * W:(j + 1) * W] = (gv * jax.nn.sigmoid(gv) * uv).astype(BF16)

            lag = jnp.where(c == 0, 3, 0)

            @pl.when((c < NC - 1) & (e == lag))
            def _():
                svc0(c + 1)

            @pl.when((c < NC - 1) & (e == lag + 1))
            def _():
                svc1(c + 1)

                @pl.when(c < NC - 2)
                def _():
                    own(c + 2)

            @pl.when((c < NC - 1) & (e == lag + 4))
            def _():
                svc2(c + 1)
            return 0

        lax.fori_loop(0, E, estep, 0)
        return 0

    lax.fori_loop(0, NC, chunk, 0)

    def dcopy(ct, buf, dev):
        return rc(pst.at[buf, 1 - k], dsum.at[ct], d_ssem.at[ct], d_rsem.at[ct], dev)

    spans = (pl.ds(0, HT), pl.ds(0, MR), pl.ds(HT, T))

    def mblock(g, i):
        x = 2 * g + i
        per = 2 * F // TC
        return x // per, pl.ds(pl.multiple_of(lax.rem(x, per) * TC, TC), TC)

    def mcopy(g, i, kind):
        e, cols = mblock(g, i)
        return rc(acc.at[e, spans[kind], cols], rmsg.at[g, i, spans[kind], :], m_ssem.at[g, i], m_rsem.at[g, i],
                  (right, left)[i])

    def mdo(g, what):
        for kind, cond in ((0, g < 2), (1, (g >= 2) & (g < NT)), (2, g >= NT)):
            @pl.when(cond)
            def _():
                for i in range(2):
                    getattr(mcopy(g, i, kind), what)()

    def svcm_new(ct):
        buf = lax.rem(ct, 2)
        dcopy(ct, buf, sib).wait_recv()
        for i, rows in ((0, lo), (1, hi)):
            e, cols = mblock(ct, i)
            acc[e, :HT, cols] = dsum[ct, oq, rows, :] + pst[buf, k, oq, rows, :]
        for d in (rq, lq, q):
            dsum[ct, d] += pst[buf, k, d]

    def svcm_old(ct):
        g = ct - 2
        mdo(g, "wait_recv")
        e, cols = mblock(ct, 0)
        acc[e, HT:2 * HT, cols] = dsum[g, rq, :HT, :] + rmsg[g, 0, :HT, :]
        acc[e, 2 * HT:MR, cols] = dsum[g, rq, HT:, :]
        e, cols = mblock(ct, 1)
        acc[e, HT:2 * HT, cols] = dsum[g, lq, :HT, :]
        acc[e, 2 * HT:MR, cols] = dsum[g, lq, HT:, :] + rmsg[g, 1, :HT, :]

    def message(ct):
        svcm_new(ct)

        @pl.when(ct >= 2)
        def _():
            svcm_old(ct)

        mdo(ct, "start")

    def svcc(ct, _):
        cols = pl.ds(pl.multiple_of(ct * TC, TC), TC)
        routed = dsum[ct, q] + rmsg[ct + 2, 0, HT:, :] + rmsg[ct + 2, 1, HT:, :]
        out_ref[:, cols] = (xown[:, cols].astype(F32) + routed + shr[:, cols].astype(F32)).astype(BF16)
        return 0

    def tile(ct, _):
        buf = lax.rem(ct, 2)
        base = n1 + 3 * ct

        def dstep(half):
            n = base + half
            sl = lax.rem(n, NS)
            wait_full(sl)
            for p in range(E // 4):
                ys = []
                for j in (2 * p, 2 * p + 1):
                    w = slots[sl, (j // 2) * F:(j // 2 + 1) * F, (j % 2) * TC:(j % 2 + 1) * TC]
                    ye = jnp.dot(h[half * (E // 2) + j], w, preferred_element_type=F32)
                    ys.append(ye.reshape(ng, cap, TC))
                y[:, half * (E // 4) + p] = jnp.concatenate(ys, axis=1).astype(BF16)
            issue(n + NS)

        dstep(0)
        dstep(1)

        @pl.when(ct >= 2)
        def _():
            dcopy(ct - 2, buf, sib).wait_send()

        def combine(b, _):
            for core in range(2):
                src = 2 * b + core
                p = jnp.dot(gt[src], y[src].reshape(E * cap, TC), preferred_element_type=F32)
                pst[buf, core, b] = p[:T] + p[T:2 * T] + p[2 * T:]
            return 0

        lax.fori_loop(0, nq, combine, 0)
        dcopy(ct, buf, sib).start()

        @pl.when(KS + ct < ns)
        def _():
            shared_step(KS + ct, base + 2)

        @pl.when(ct >= 1)
        def _():
            message(ct - 1)
        return 0

    lax.fori_loop(0, NT, tile, 0)
    message(jnp.int32(NT - 1))
    for g in (NT, NT + 1):
        svcm_old(jnp.int32(g))
        mdo(jnp.int32(g), "start")
    lax.fori_loop(0, NT - 2, svcc, 0)
    for g in (NT, NT + 1):
        mdo(jnp.int32(g), "wait_recv")
        svcc(jnp.int32(g - 2), 0)

    for i in range(1, ng):
        d = lax.rem(me + i, ng)
        rc(gsend.at[d], grecv.at[me], g_ssem.at[i], g_rsem.at[i], d).wait_send()

    def drain_ag(c, _):
        for typ, rows in ((0, lo), (1, hi), (2, hi), (3, lo), (4, lo), (5, hi), (6, None), (7, None), (8, None), (9, None)):
            ag(c, typ, sib, me, rows).wait_send()
        return 0

    lax.fori_loop(0, NC, drain_ag, 0)

    def drain_rs(ct, _):
        @pl.when((ct >= NT - 2) & (ct < NT))
        def _():
            dcopy(ct, lax.rem(ct, 2), sib).wait_send()
        mdo(ct, "wait_send")
        return 0

    lax.fori_loop(0, nm, drain_rs, 0)


def solution(mesh):
    ng = mesh.shape["ep"]
    nq = ng // 2

    def moe_step(tokens, expert_ids, gate_vals, w_gate, w_up, w_down, shared_gate, shared_up, shared_down):
        T, D = tokens.shape
        top = expert_ids.shape[1]
        E, _, F = w_gate.shape
        SF = shared_gate.shape[1]
        spread = max(ng, E * ng // 2)
        cap = (T * top + spread - 1) // spread
        W = D // NC
        TC = W // 2
        NT = D // TC
        R = 2 * cap
        M = nq * R
        dims = (ng, nq, T, D, F, SF, E, cap, top)
        any_spec = pl.BlockSpec(memory_space=pl.ANY)
        vm_spec = pl.BlockSpec(memory_space=pltpu.VMEM)
        dma = pltpu.SemaphoreType.DMA
        flops = 2 * 3 * D * (E * M * F + T * SF)
        return pl.pallas_call(
            functools.partial(moe_kernel, dims),
            out_shape=jax.ShapeDtypeStruct((T, D), BF16),
            in_specs=[vm_spec, vm_spec] + [any_spec] * 7,
            out_specs=vm_spec,
            scratch_shapes=[
                pltpu.VMEM((NC, ng, T, W), BF16),
                pltpu.VMEM((T, D), BF16),
                pltpu.VMEM((E, M, W), BF16),
                pltpu.VMEM((E, M, 2 * F), F32),
                pltpu.VMEM((E, M, F), BF16),
                pltpu.VMEM((ng, E // 2, R, TC), BF16),
                pltpu.VMEM((2, 2, nq, T, TC), F32),
                pltpu.VMEM((NT, nq, T, TC), F32),
                pltpu.VMEM((NT + 2, 2, T + T // 2, TC), F32),
                pltpu.VMEM((nq, E, R, 2 * T), BF16),
                pltpu.VMEM((ng, 3 * T, E * cap), BF16),
                pltpu.VMEM((T, SF), BF16),
                pltpu.VMEM((T, W), F32),
                pltpu.VMEM((T, D), BF16),
                pltpu.VMEM((ng, E, T), F32),
                pltpu.VMEM((ng, E, T), F32),
                pltpu.VMEM((ng, E, T), F32),
                pltpu.VMEM((NS, SF, W), BF16),
                dma((NS,)), dma((NC + 1,)), dma((ng,)), dma((ng,)),
                dma((NC, 10)), dma((NC, 10)), dma((NT,)), dma((NT,)),
                dma((NT + 2, 2)), dma((NT + 2, 2)),
            ],
            compiler_params=pltpu.CompilerParams(collective_id=0, has_side_effects=True, vmem_limit_bytes=67043328),
            cost_estimate=pl.CostEstimate(flops=flops, bytes_accessed=2 * 3 * D * (E * F + SF), transcendentals=0),
        )(expert_ids.T, gate_vals.T, tokens, w_gate, w_up, w_down, shared_gate, shared_up, shared_down)

    row_spec = P(("dp", "ep"), None)
    expert_spec = P("ep", None, None)
    whole_spec = P(None, None)
    return jax.shard_map(moe_step, mesh=mesh, in_specs=(row_spec, row_spec, row_spec, expert_spec, expert_spec, expert_spec, whole_spec, whole_spec, whole_spec), out_specs=row_spec, check_vma=False)
```

```python
import functools

import jax
import jax.numpy as jnp
from jax import lax
from jax.experimental import pallas as pl
from jax.experimental.pallas import tpu as pltpu
from jax.sharding import PartitionSpec as P

F32 = jnp.float32
BF16 = jnp.bfloat16
NS = 5
NC = 5
KS = 8


def moe_kernel(dims, ids_ref, gates_ref, tok, wg, wu, wd, sg, su, sd, out_ref,
               xall, xown, xg, acc, h, y, pst, dsum, rmsg, oh, gt, hs, sgacc, shr, posr, grecv, gsend, slots,
               slot_sem, loc_sem, g_ssem, g_rsem, a_ssem, a_rsem, d_ssem, d_rsem, m_ssem, m_rsem):
    ng, nq, T, D, F, SF, E, cap, top = dims
    W = D // NC
    TC = W // 2
    NT = D // TC
    R = 2 * cap
    M = nq * R
    HT = T // 2
    FJ = F // W
    SFJ = SF // W
    n1 = KS + NC * E
    ns = 2 * SFJ + NC
    n2 = n1 + 2 * NT
    ntot = n2 + ns - KS
    nm = NT + 2
    MR = HT + T

    me = lax.axis_index("ep")
    q = me // 2
    k = lax.rem(me, 2)
    lq = lax.rem(q + nq - 1, nq)
    rq = lax.rem(q + 1, nq)
    oq = lax.rem(q + 2, nq)
    sib = 2 * q + 1 - k
    left = 2 * lq + k
    right = 2 * rq + k
    opp = 2 * oq + k

    def rc(src, dst, ssem, rsem, dev):
        return pltpu.make_async_remote_copy(src_ref=src, dst_ref=dst, send_sem=ssem, recv_sem=rsem,
                                            device_id={"ep": dev}, device_id_type=pl.DeviceIdType.MESH)

    def issue(n):
        sl = lax.rem(n, NS)
        sem = slot_sem.at[sl]

        @pl.when((n >= KS) & (n < n1))
        def _():
            c = (n - KS) // E
            e = lax.rem(n - KS, E)
            for j in range(FJ):
                pltpu.make_async_copy(wg.at[e, pl.ds(pl.multiple_of(c * W, W), W), pl.ds(j * W, W)],
                                      slots.at[sl, pl.ds(j * W, W), :], sem).start()
            for j in range(FJ):
                pltpu.make_async_copy(wu.at[e, pl.ds(pl.multiple_of(c * W, W), W), pl.ds(j * W, W)],
                                      slots.at[sl, pl.ds((FJ + j) * W, W), :], sem).start()

        m = jnp.maximum(n - n1, 0)
        ct = m // 2
        half = lax.rem(m, 2)

        @pl.when((n >= n1) & (n < n2))
        def _():
            for j in range(E // 2):
                pltpu.make_async_copy(wd.at[half * (E // 2) + j, :, pl.ds(pl.multiple_of(ct * TC, TC), TC)],
                                      slots.at[sl, pl.ds((j // 2) * F, F), pl.ds((j % 2) * TC, TC)], sem).start()

        s = jnp.where(n < KS, n, n - n2 + KS)
        shared = (n < KS) | ((n >= n2) & (n < ntot))
        fcol = pl.ds(pl.multiple_of((s // 2) * W, W), W)

        @pl.when(shared & (s < 2 * SFJ) & (lax.rem(s, 2) == 0))
        def _():
            pltpu.make_async_copy(sg.at[:, fcol], slots.at[sl, pl.ds(0, D), :], sem).start()

        @pl.when(shared & (s < 2 * SFJ) & (lax.rem(s, 2) == 1))
        def _():
            pltpu.make_async_copy(su.at[:, fcol], slots.at[sl, pl.ds(0, D), :], sem).start()

        @pl.when(shared & (s >= 2 * SFJ))
        def _():
            col = pl.ds(pl.multiple_of((s - 2 * SFJ) * W, W), W)
            pltpu.make_async_copy(sd.at[:, col], slots.at[sl], sem).start()

    def wait_full(sl):
        pltpu.make_async_copy(sd.at[:, pl.ds(0, W)], slots.at[sl], slot_sem.at[sl]).wait()

    def wait_gu(sl):
        pltpu.make_async_copy(sg.at[:, pl.ds(0, W)], slots.at[sl, pl.ds(0, D), :], slot_sem.at[sl]).wait()

    xcopies = [pltpu.make_async_copy(tok.at[:, pl.ds(c * W, W)], xall.at[c, me], loc_sem.at[c]) for c in range(NC)]
    xcopies.append(pltpu.make_async_copy(tok, xown, loc_sem.at[NC]))
    for cp in xcopies:
        cp.start()
    for n in range(NS):
        issue(jnp.int32(n))

    eiota = lax.broadcasted_iota(jnp.int32, (ng * E, T), 0)
    dense = jnp.zeros((ng * E, T), F32)
    for j in range(top):
        dense = dense + jnp.where(ids_ref[j:j + 1, :] == eiota, gates_ref[j:j + 1, :], 0.0)
    gsend[...] = dense.reshape(ng, E, T)

    bar = pltpu.get_barrier_semaphore()
    for i in range(1, ng):
        pl.semaphore_signal(bar, inc=1, device_id={"ep": lax.rem(me + i, ng)}, device_id_type=pl.DeviceIdType.MESH)
    pl.semaphore_wait(bar, ng - 1)

    lo, hi = pl.ds(0, HT), pl.ds(HT, HT)

    def ag(c, typ, dev, src_dev, rows, dst_dev=None):
        ref = xall.at[c, src_dev] if rows is None else xall.at[c, src_dev, rows, :]
        return rc(ref, ref, a_ssem.at[c, typ], a_rsem.at[c, typ], dev)

    def own(c):
        ag(c, 0, right, me, lo).start()
        ag(c, 2, left, me, hi).start()
        ag(c, 1, right, me, hi).start()
        ag(c, 3, left, me, lo).start()
        ag(c, 6, sib, me, None).start()

    def svc0(c):
        ag(c, 0, left, left, lo).wait_recv()
        ag(c, 4, right, left, lo).start()
        ag(c, 2, right, right, hi).wait_recv()
        ag(c, 5, left, right, hi).start()

    def svc1(c):
        ag(c, 1, left, left, hi).wait_recv()
        ag(c, 7, sib, left, None).start()
        ag(c, 3, right, right, lo).wait_recv()
        ag(c, 8, sib, right, None).start()

    def svc2(c):
        ag(c, 4, left, opp, lo).wait_recv()
        ag(c, 5, right, opp, hi).wait_recv()
        ag(c, 9, sib, opp, None).start()

    def need(c):
        sl_, sr_, so_ = 2 * lq + 1 - k, 2 * rq + 1 - k, 2 * oq + 1 - k
        ag(c, 6, sib, sib, None).wait_recv()
        ag(c, 7, sib, sl_, None).wait_recv()
        ag(c, 8, sib, sr_, None).wait_recv()
        ag(c, 9, sib, so_, None).wait_recv()

    def shared_gu(s, n):
        sl = lax.rem(n, NS)
        fcol = pl.ds(pl.multiple_of((s // 2) * W, W), W)

        @pl.when(lax.rem(s, 2) == 0)
        def _():
            wait_gu(sl)
            sgacc[...] = jnp.dot(xown[...], slots[sl, :D, :], preferred_element_type=F32)

        @pl.when(lax.rem(s, 2) == 1)
        def _():
            wait_gu(sl)
            uv = jnp.dot(xown[...], slots[sl, :D, :], preferred_element_type=F32)
            gv = sgacc[...]
            hs[:, fcol] = (gv * jax.nn.sigmoid(gv) * uv).astype(BF16)

    def shared_step(s, n):
        sl = lax.rem(n, NS)

        @pl.when(s < 2 * SFJ)
        def _():
            shared_gu(s, n)

        @pl.when(s >= 2 * SFJ)
        def _():
            wait_full(sl)
            col = pl.ds(pl.multiple_of((s - 2 * SFJ) * W, W), W)
            shr[:, col] = jnp.dot(hs[...], slots[sl], preferred_element_type=F32).astype(BF16)

        issue(n + NS)

    def early(first, last):
        def body(n, _):
            shared_gu(n, n)
            issue(n + NS)
            return 0
        lax.fori_loop(first, last, body, 0)

    for c in range(NC):
        xcopies[c].wait()
    own(jnp.int32(0))
    for i in range(1, ng):
        d = lax.rem(me + i, ng)
        rc(gsend.at[d], grecv.at[me], g_ssem.at[i], g_rsem.at[i], d).start()

    xcopies[NC].wait()
    early(0, 3)
    for e in range(E):
        acc[e] = jnp.zeros((M, 2 * F), F32)
    early(3, 4)
    svc0(jnp.int32(0))
    early(4, 5)
    svc1(jnp.int32(0))

    for i in range(1, ng):
        s = lax.rem(me + ng - i, ng)
        rc(gsend.at[s], grecv.at[s], g_ssem.at[i], g_rsem.at[i], s).wait_recv()
    grecv[me] = gsend[me]
    gall = grecv[...].reshape(ng * E, T)
    mask = gall > 0.0
    tri = (lax.broadcasted_iota(jnp.int32, (T, T), 0) < lax.broadcasted_iota(jnp.int32, (T, T), 1)).astype(F32).astype(BF16)
    pos = jnp.dot(mask.astype(F32).astype(BF16), tri, preferred_element_type=F32)
    posr[...] = jnp.where(mask, pos, -1000.0).reshape(ng, E, T)

    riota = lax.broadcasted_iota(jnp.int32, (R, T), 0).astype(F32)
    ciota = lax.broadcasted_iota(jnp.int32, (cap, T), 0).astype(F32)

    def route(b, _):
        for e in range(E):
            hits = [jnp.where(posr[2 * b + s, e:e + 1, :] == (riota - float(s * cap)), 1.0, 0.0) for s in range(2)]
            oh[b, e] = jnp.concatenate(hits, axis=1).astype(BF16)
        for s in range(2):
            src = 2 * b + s
            g = jnp.concatenate([jnp.where(posr[src, e:e + 1, :] == ciota, grecv[src, e:e + 1, :], 0.0)
                                 for e in range(E)], axis=0).T
            g0 = g.astype(BF16)
            rem = g - g0.astype(F32)
            g1 = rem.astype(BF16)
            gt[src, :T] = g0
            gt[src, T:2 * T] = g1
            gt[src, 2 * T:] = (rem - g1.astype(F32)).astype(BF16)
        return 0

    lax.fori_loop(0, nq, route, 0)
    early(5, 6)
    svc2(jnp.int32(0))
    own(jnp.int32(1))
    early(6, KS)

    def chunk(c, _):
        need(c)
        for b in range(nq):
            ohb = oh[b].reshape(E * R, 2 * T)
            xb = xall[c, 2 * b:2 * b + 2].reshape(2 * T, W)
            rows = jnp.dot(ohb, xb, preferred_element_type=F32).astype(BF16)
            xg[:, b * R:(b + 1) * R, :] = rows.reshape(E, R, W)

        def estep(e, _):
            n = KS + c * E + e
            sl = lax.rem(n, NS)
            wait_full(sl)
            xe = xg[e]
            for j in range(2 * FJ):
                acc[e, :, j * W:(j + 1) * W] += jnp.dot(xe, slots[sl, j * W:(j + 1) * W, :], preferred_element_type=F32)
            issue(n + NS)

            @pl.when(c == NC - 1)
            def _():
                for j in range(FJ):
                    gv = acc[e, :, j * W:(j + 1) * W]
                    uv = acc[e, :, F + j * W:F + (j + 1) * W]
                    h[e, :, j * W:(j + 1) * W] = (gv * jax.nn.sigmoid(gv) * uv).astype(BF16)

            lag = jnp.where(c == 0, 3, 0)

            @pl.when((c < NC - 1) & (e == lag))
            def _():
                svc0(c + 1)

            @pl.when((c < NC - 1) & (e == lag + 1))
            def _():
                svc1(c + 1)

                @pl.when(c < NC - 2)
                def _():
                    own(c + 2)

            @pl.when((c < NC - 1) & (e == lag + 4))
            def _():
                svc2(c + 1)
            return 0

        lax.fori_loop(0, E, estep, 0)
        return 0

    lax.fori_loop(0, NC, chunk, 0)

    def dcopy(ct, buf, dev):
        return rc(pst.at[buf, 1 - k], dsum.at[ct], d_ssem.at[ct], d_rsem.at[ct], dev)

    spans = (pl.ds(0, HT), pl.ds(0, MR), pl.ds(HT, T))

    def mblock(g, i):
        x = 2 * g + i
        per = 2 * F // TC
        return x // per, pl.ds(pl.multiple_of(lax.rem(x, per) * TC, TC), TC)

    def mcopy(g, i, kind):
        e, cols = mblock(g, i)
        return rc(acc.at[e, spans[kind], cols], rmsg.at[g, i, spans[kind], :], m_ssem.at[g, i], m_rsem.at[g, i],
                  (right, left)[i])

    def mdo(g, what):
        for kind, cond in ((0, g < 2), (1, (g >= 2) & (g < NT)), (2, g >= NT)):
            @pl.when(cond)
            def _():
                for i in range(2):
                    getattr(mcopy(g, i, kind), what)()

    def svcm_new(ct):
        buf = lax.rem(ct, 2)
        dcopy(ct, buf, sib).wait_recv()
        for i, rows in ((0, lo), (1, hi)):
            e, cols = mblock(ct, i)
            acc[e, :HT, cols] = dsum[ct, oq, rows, :] + pst[buf, k, oq, rows, :]
        for d in (rq, lq, q):
            dsum[ct, d] += pst[buf, k, d]

    def svcm_old(ct):
        g = ct - 2
        mdo(g, "wait_recv")
        e, cols = mblock(ct, 0)
        acc[e, HT:2 * HT, cols] = dsum[g, rq, :HT, :] + rmsg[g, 0, :HT, :]
        acc[e, 2 * HT:MR, cols] = dsum[g, rq, HT:, :]
        e, cols = mblock(ct, 1)
        acc[e, HT:2 * HT, cols] = dsum[g, lq, :HT, :]
        acc[e, 2 * HT:MR, cols] = dsum[g, lq, HT:, :] + rmsg[g, 1, :HT, :]

    def message(ct):
        svcm_new(ct)

        @pl.when(ct >= 2)
        def _():
            svcm_old(ct)

        mdo(ct, "start")

    def svcc(ct, _):
        cols = pl.ds(pl.multiple_of(ct * TC, TC), TC)
        routed = dsum[ct, q] + rmsg[ct + 2, 0, HT:, :] + rmsg[ct + 2, 1, HT:, :]
        out_ref[:, cols] = (xown[:, cols].astype(F32) + routed + shr[:, cols].astype(F32)).astype(BF16)
        return 0

    def tile(ct, _):
        buf = lax.rem(ct, 2)
        base = n1 + 2 * ct

        def dstep(half):
            n = base + half
            sl = lax.rem(n, NS)
            wait_full(sl)
            for p in range(E // 4):
                ys = []
                for j in (2 * p, 2 * p + 1):
                    w = slots[sl, (j // 2) * F:(j // 2 + 1) * F, (j % 2) * TC:(j % 2 + 1) * TC]
                    ye = jnp.dot(h[half * (E // 2) + j], w, preferred_element_type=F32)
                    ys.append(ye.reshape(ng, cap, TC))
                y[:, half * (E // 4) + p] = jnp.concatenate(ys, axis=1).astype(BF16)
            issue(n + NS)

        dstep(0)
        dstep(1)

        @pl.when(ct >= 2)
        def _():
            dcopy(ct - 2, buf, sib).wait_send()

        def combine(b, _):
            for core in range(2):
                src = 2 * b + core
                p = jnp.dot(gt[src], y[src].reshape(E * cap, TC), preferred_element_type=F32)
                pst[buf, core, b] = p[:T] + p[T:2 * T] + p[2 * T:]
            return 0

        lax.fori_loop(0, nq, combine, 0)
        dcopy(ct, buf, sib).start()

        @pl.when(ct >= 1)
        def _():
            message(ct - 1)
        return 0

    lax.fori_loop(0, NT, tile, 0)
    message(jnp.int32(NT - 1))

    def tail(i, _):
        shared_step(KS + i, n2 + i)

        @pl.when((i == 2) | (i == 5))
        def _():
            g = NT + i // 3
            svcm_old(g)
            mdo(g, "start")
        return 0

    lax.fori_loop(0, ns - KS, tail, 0)
    lax.fori_loop(0, NT - 2, svcc, 0)
    for g in (NT, NT + 1):
        mdo(jnp.int32(g), "wait_recv")
        svcc(jnp.int32(g - 2), 0)

    for i in range(1, ng):
        d = lax.rem(me + i, ng)
        rc(gsend.at[d], grecv.at[me], g_ssem.at[i], g_rsem.at[i], d).wait_send()

    def drain_ag(c, _):
        for typ, rows in ((0, lo), (1, hi), (2, hi), (3, lo), (4, lo), (5, hi), (6, None), (7, None), (8, None), (9, None)):
            ag(c, typ, sib, me, rows).wait_send()
        return 0

    lax.fori_loop(0, NC, drain_ag, 0)

    def drain_rs(ct, _):
        @pl.when((ct >= NT - 2) & (ct < NT))
        def _():
            dcopy(ct, lax.rem(ct, 2), sib).wait_send()
        mdo(ct, "wait_send")
        return 0

    lax.fori_loop(0, nm, drain_rs, 0)


def solution(mesh):
    ng = mesh.shape["ep"]
    nq = ng // 2

    def moe_step(tokens, expert_ids, gate_vals, w_gate, w_up, w_down, shared_gate, shared_up, shared_down):
        T, D = tokens.shape
        top = expert_ids.shape[1]
        E, _, F = w_gate.shape
        SF = shared_gate.shape[1]
        spread = max(ng, E * ng // 2)
        cap = (T * top + spread - 1) // spread
        W = D // NC
        TC = W // 2
        NT = D // TC
        R = 2 * cap
        M = nq * R
        dims = (ng, nq, T, D, F, SF, E, cap, top)
        any_spec = pl.BlockSpec(memory_space=pl.ANY)
        vm_spec = pl.BlockSpec(memory_space=pltpu.VMEM)
        dma = pltpu.SemaphoreType.DMA
        flops = 2 * 3 * D * (E * M * F + T * SF)
        return pl.pallas_call(
            functools.partial(moe_kernel, dims),
            out_shape=jax.ShapeDtypeStruct((T, D), BF16),
            in_specs=[vm_spec, vm_spec] + [any_spec] * 7,
            out_specs=vm_spec,
            scratch_shapes=[
                pltpu.VMEM((NC, ng, T, W), BF16),
                pltpu.VMEM((T, D), BF16),
                pltpu.VMEM((E, M, W), BF16),
                pltpu.VMEM((E, M, 2 * F), F32),
                pltpu.VMEM((E, M, F), BF16),
                pltpu.VMEM((ng, E // 2, R, TC), BF16),
                pltpu.VMEM((2, 2, nq, T, TC), F32),
                pltpu.VMEM((NT, nq, T, TC), F32),
                pltpu.VMEM((NT + 2, 2, T + T // 2, TC), F32),
                pltpu.VMEM((nq, E, R, 2 * T), BF16),
                pltpu.VMEM((ng, 3 * T, E * cap), BF16),
                pltpu.VMEM((T, SF), BF16),
                pltpu.VMEM((T, W), F32),
                pltpu.VMEM((T, D), BF16),
                pltpu.VMEM((ng, E, T), F32),
                pltpu.VMEM((ng, E, T), F32),
                pltpu.VMEM((ng, E, T), F32),
                pltpu.VMEM((NS, SF, W), BF16),
                dma((NS,)), dma((NC + 1,)), dma((ng,)), dma((ng,)),
                dma((NC, 10)), dma((NC, 10)), dma((NT,)), dma((NT,)),
                dma((NT + 2, 2)), dma((NT + 2, 2)),
            ],
            compiler_params=pltpu.CompilerParams(collective_id=0, has_side_effects=True, vmem_limit_bytes=67043328),
            cost_estimate=pl.CostEstimate(flops=flops, bytes_accessed=2 * 3 * D * (E * F + SF), transcendentals=0),
        )(expert_ids.T, gate_vals.T, tokens, w_gate, w_up, w_down, shared_gate, shared_up, shared_down)

    row_spec = P(("dp", "ep"), None)
    expert_spec = P("ep", None, None)
    whole_spec = P(None, None)
    return jax.shard_map(moe_step, mesh=mesh, in_specs=(row_spec, row_spec, row_spec, expert_spec, expert_spec, expert_spec, whole_spec, whole_spec, whole_spec), out_specs=row_spec, check_vma=False)
```
